32 devices in a mesh: blk: 8 (over z, x), lane: 4 (over y, core).
Axes of the slice: x: 2, y: 2, z: 4, core: 2. Of those that a mesh axis runs over, the one named last changes fastest.
Arguments:
- left_factor: bfloat16 [4096, 512], P('blk'), may hold values from -6 to 6
- right_factor: bfloat16 [4, 4096, 512], P('lane', 'blk'), may hold values from -6 to 6
- observed: bfloat16 [4, 4, 512, 4096], P('lane', None, None, 'blk'), may hold values from -6 to 6
- row_codes: int32 [4096], P('blk'), may hold values from 0 to 1073741823
- shift_codes: int32 [4, 4, 4096], P('lane', None, 'blk'), may hold values from 0 to 29
Outputs:
- left_out: bfloat16 [4096, 512], P('blk')
- right_out: bfloat16 [4, 4096, 512], P('lane', 'blk')
The draws below stay inside these ranges and needn't reach their ends.
Inputs may be any that keep to these rules, and one draw needn't show every extreme that they name: `row_codes`: each row's word carries thirty independent sampling bits. `shift_codes`: A bit number for each lane, cycle step and visited tile entry column.
All inputs are finite; a program needn't handle non-finite values.
Results may differ from the reference program's by a relative error of at most 0.013.
Values may be sent and summed in bfloat16 or wider, within the bound.
A program may use at most 64 MiB of HBM per device.

```python
import math
import jax
import jax.numpy as jnp
from jax import lax

RANK = 512
TILE_COLS = 512
TILE_ROWS = 512
STEPS = 4
BLOCKS = 8
ROWS = 4096
COLUMNS = 4096
N_LANE = 4


def touch_ends(drawn, rng, low, high):
    longest = drawn.shape.index(max(drawn.shape))
    spots = []
    for shift in (0, 1):
        where = [jax.random.randint(jax.random.fold_in(rng, axis), (), 0, length) for axis, length in enumerate(drawn.shape)]
        where[longest] = (where[longest] + shift) % drawn.shape[longest]
        spots.append(tuple(where))
    return drawn.at[spots[0]].set(low).at[spots[1]].set(high)


def steps_of(rng, shape, pieces, smallest, high):
    gain = 1.0
    for axis_at, shards_of in pieces:
        steps = jax.random.uniform(jax.random.fold_in(jax.random.fold_in(rng, 6), axis_at), (shards_of,), jnp.float32, smallest / len(pieces), high / len(pieces))
        gain = gain * jnp.repeat(jnp.exp(steps), shape[axis_at] // shards_of).reshape((-1,) + (1,) * (len(shape) - 1 - axis_at))
    return gain


def normal_values(rng, dims, scale, reach, split=(), kind=jnp.bfloat16):
    drawn = jax.random.normal(rng, dims, jnp.float32) * scale
    if len(split) > 0:
        drawn = steps_of(rng, dims, split, -0.22, 0.18) * drawn
    return jnp.clip(drawn, min=-reach, max=reach).astype(kind)


def setup_inputs(seed: int = 0) -> dict:
    key_list = jax.random.split(jax.random.key(seed), 6)
    left_factor = normal_values(key_list[0], (ROWS, RANK), 1.0, 6.0, ((0, 8),))
    right_factor = normal_values(key_list[1], (N_LANE, COLUMNS, RANK), 1.0, 6.0, ((0, 4), (1, 8)))
    observed = normal_values(key_list[2], (N_LANE, STEPS, TILE_COLS, ROWS), 1.0, 6.0, ((0, 4), (3, 8)))
    row_codes = touch_ends(jax.random.randint(key_list[3], (ROWS,), 0, 1073741824), jax.random.fold_in(key_list[3], 1), 0, 1073741823).astype(jnp.int32)
    shift_codes = touch_ends(jax.random.randint(key_list[4], (N_LANE, STEPS, COLUMNS), 0, 30), jax.random.fold_in(key_list[4], 1), 0, 29).astype(jnp.int32)
    return {"left_factor": left_factor, "right_factor": right_factor, "observed": observed, "row_codes": row_codes, "shift_codes": shift_codes}


step_right = 0.25
step_left = 0.1

def reference(left_factor, right_factor, observed, row_codes, shift_codes):
    root_scale = 1.0 / math.sqrt(RANK)
    left_blocks = left_factor.reshape(BLOCKS, TILE_ROWS, RANK).astype(jnp.float32)
    row_blocks = row_codes.reshape(BLOCKS, TILE_ROWS)
    grad_total = jnp.zeros((BLOCKS, TILE_ROWS, RANK), jnp.float32)
    right_list = []
    for lane_index in range(N_LANE):
        right_now = right_factor[lane_index].reshape(BLOCKS, TILE_COLS, RANK)
        for cycle_step in range(STEPS):
            visited = jnp.roll(right_now, cycle_step, axis=0).astype(jnp.float32)
            predicted = jnp.einsum('nck,nrk->ncr', visited, left_blocks) * root_scale
            shifts = shift_codes[lane_index, cycle_step].reshape(BLOCKS, TILE_COLS)
            sample_bits = jnp.right_shift(row_blocks[:, None, :], shifts[:, :, None]) & 1
            target = observed[lane_index, cycle_step].reshape(TILE_COLS, BLOCKS, TILE_ROWS)
            target = jnp.transpose(target, (1, 0, 2)).astype(jnp.float32)
            error_tile = jnp.where(sample_bits == 1, predicted - target, 0.0).astype(jnp.bfloat16)
            error_tile = lax.optimization_barrier(error_tile).astype(jnp.float32)
            grad_right = jnp.einsum('ncr,nrk->nck', error_tile, left_blocks)
            grad_total = grad_total + jnp.einsum('ncr,nck->nrk', error_tile, visited)
            updated = (visited - step_right * root_scale * grad_right).astype(jnp.bfloat16)
            right_now = jnp.roll(updated, -cycle_step, axis=0)
        placed = jnp.roll(right_now, STEPS - 1, axis=0)
        right_list.append(placed.reshape(BLOCKS * TILE_COLS, RANK))
    left_out = (left_blocks - step_left * root_scale * grad_total).astype(jnp.bfloat16)
    return (left_out.reshape(BLOCKS * TILE_ROWS, RANK), jnp.stack(right_list))
```

```python
import functools
import math

import jax
import jax.numpy as jnp
from jax import lax
from jax.experimental import pallas as pl
from jax.experimental.pallas import tpu as pltpu
from jax.sharding import PartitionSpec as P

step_right = 0.25
step_left = 0.1

CHUNKS = 4
PIECES = 4
MESH = pl.DeviceIdType.MESH


def kernel(
    blocks, lanes,
    left_hbm, right_hbm, obs_hbm, codes_ref, shift_ref,
    left_out, right_out,
    left, visited, updated, obs, grad, pair_out, pair_in, peer_out, peer_in, result,
    load_sem, send_sem, recv_sem, store_sem, pair_send, pair_recv, peer_send, peer_recv, last_send, last_recv, out_sem,
):
    steps, cols, rows = obs.shape
    rank = left.shape[1]
    scale = 1.0 / math.sqrt(rank)
    size = cols // CHUNKS
    half = rows // 2
    part = half // PIECES
    blk = lax.axis_index("blk")
    lane = lax.axis_index("lane")
    ahead = lax.rem(blk + 1, blocks)
    behind = lax.rem(blk + blocks - 1, blocks)
    side = lax.rem(lane, 2)
    pair = lane + 1 - 2 * side
    peers = [lax.rem(lane + 2 * hop, lanes) for hop in range(1, lanes // 2)]

    loads = [
        pltpu.make_async_copy(left_hbm, left, load_sem.at[0]),
        pltpu.make_async_copy(right_hbm.at[0], visited.at[0], load_sem.at[1]),
    ]
    for s in range(steps):
        loads.append(pltpu.make_async_copy(obs_hbm.at[0, s], obs.at[s], load_sem.at[2 + s]))
    for copy in loads:
        copy.start()

    barrier = pltpu.get_barrier_semaphore()
    for neighbour in (behind, ahead):
        pl.semaphore_signal(barrier, inc=1, device_id={"blk": neighbour}, device_id_type=MESH)
    for friend in [pair] + peers:
        pl.semaphore_signal(barrier, inc=1, device_id={"lane": friend}, device_id_type=MESH)
    pl.semaphore_wait(barrier, 2 + 1 + len(peers))

    grad[...] = jnp.zeros_like(grad)
    loads[0].wait()
    loads[1].wait()

    def hop(s, k):
        span = pl.ds(pl.multiple_of(k * size, size), size)
        return pltpu.make_async_remote_copy(
            src_ref=updated.at[s, span],
            dst_ref=visited.at[s + 1, span],
            send_sem=send_sem.at[s, k],
            recv_sem=recv_sem.at[s, k],
            device_id={"blk": ahead},
            device_id_type=MESH,
        )

    def keep(k):
        span = pl.ds(pl.multiple_of(k * size, size), size)
        return pltpu.make_async_copy(updated.at[steps - 1, span], right_out.at[0, span], store_sem.at[k])

    for s in range(steps):
        loads[2 + s].wait()

        @pl.loop(0, CHUNKS)
        def _(k):
            span = pl.ds(pl.multiple_of(k * size, size), size)
            shifts = jnp.transpose(jnp.broadcast_to(shift_ref[s, pl.ds(k, 1), :], (size, size)))
            shifts = jnp.concatenate([shifts] * (rows // size), axis=1)
            seen = (jnp.right_shift(codes_ref[...], shifts) & 1) == 1
            if s > 0:
                hop(s - 1, k).wait_recv()
            block = visited[s, span, :]
            predicted = lax.dot_general(
                block, left[...], (((1,), (1,)), ((), ())), preferred_element_type=jnp.float32
            )
            error = predicted * scale - obs[s, span, :].astype(jnp.float32)
            error = jnp.where(seen, error, 0.0).astype(jnp.bfloat16)
            move = jnp.dot(error, left[...], preferred_element_type=jnp.float32)
            updated[s, span, :] = (block.astype(jnp.float32) - step_right * scale * move).astype(jnp.bfloat16)
            if s + 1 < steps:
                hop(s, k).start()
            else:
                keep(k).start()
            grad[...] += lax.dot_general(
                error, block, (((0,), (0,)), ((), ())), preferred_element_type=jnp.float32
            )

    mine = pl.multiple_of(side * half, half)
    other = pl.multiple_of((1 - side) * half, half)

    def swap(q):
        span = pl.ds(q * part, part)
        return pltpu.make_async_remote_copy(
            src_ref=pair_out.at[span], dst_ref=pair_in.at[span],
            send_sem=pair_send.at[q], recv_sem=pair_recv.at[q],
            device_id={"lane": pair}, device_id_type=MESH,
        )

    def cross(m, q):
        span = pl.ds(q * part, part)
        return pltpu.make_async_remote_copy(
            src_ref=peer_out.at[span], dst_ref=peer_in.at[m, span],
            send_sem=peer_send.at[m, q], recv_sem=peer_recv.at[m, q],
            device_id={"lane": peers[m]}, device_id_type=MESH,
        )

    def share(q):
        span = pl.ds(pl.multiple_of(mine + q * part, part), part)
        return pltpu.make_async_remote_copy(
            src_ref=result.at[span], dst_ref=result.at[span],
            send_sem=last_send.at[q], recv_sem=last_recv.at[q],
            device_id={"lane": pair}, device_id_type=MESH,
        )

    for q in range(PIECES):
        pair_out[pl.ds(q * part, part), :] = grad[pl.ds(pl.multiple_of(other + q * part, part), part), :].astype(jnp.bfloat16)
        swap(q).start()
    for q in range(PIECES):
        span = pl.ds(q * part, part)
        swap(q).wait_recv()
        peer_out[span, :] = (
            grad[pl.ds(pl.multiple_of(mine + q * part, part), part), :] + pair_in[span, :].astype(jnp.float32)
        ).astype(jnp.bfloat16)
        for m in range(len(peers)):
            cross(m, q).start()
    for q in range(PIECES):
        span = pl.ds(q * part, part)
        here = pl.ds(pl.multiple_of(mine + q * part, part), part)
        total = peer_out[span, :].astype(jnp.float32)
        for m in range(len(peers)):
            cross(m, q).wait_recv()
            total = total + peer_in[m, span, :].astype(jnp.float32)
        result[here, :] = (left[here, :].astype(jnp.float32) - step_left * scale * total).astype(jnp.bfloat16)
        share(q).start()
    own = pltpu.make_async_copy(result.at[pl.ds(mine, half)], left_out.at[pl.ds(mine, half)], out_sem.at[0])
    own.start()
    for q in range(PIECES):
        share(q).wait_recv()
    theirs = pltpu.make_async_copy(result.at[pl.ds(other, half)], left_out.at[pl.ds(other, half)], out_sem.at[1])
    theirs.start()
    for s in range(steps - 1):
        @pl.loop(0, CHUNKS)
        def _(k):
            hop(s, k).wait_send()

    @pl.loop(0, CHUNKS)
    def _(k):
        keep(k).wait()

    for q in range(PIECES):
        swap(q).wait_send()
        for m in range(len(peers)):
            cross(m, q).wait_send()
        share(q).wait_send()
    own.wait()
    theirs.wait()


def solution(mesh):
    blocks = mesh.shape["blk"]
    lanes = mesh.shape["lane"]

    def local(left_factor, right_factor, observed, row_codes, shift_codes):
        rows, rank = left_factor.shape
        _, steps, cols, _ = observed.shape
        size = cols // CHUNKS
        bf16, f32 = jnp.bfloat16, jnp.float32
        dma = pltpu.SemaphoreType.DMA
        anywhere = pl.BlockSpec(memory_space=pl.ANY)
        vmem = pl.BlockSpec(memory_space=pltpu.VMEM)
        others = lanes // 2 - 1
        return pl.pallas_call(
            functools.partial(kernel, blocks, lanes),
            out_shape=(
                jax.ShapeDtypeStruct((rows, rank), bf16),
                jax.ShapeDtypeStruct((1, cols, rank), bf16),
            ),
            in_specs=[anywhere, anywhere, anywhere, vmem, vmem],
            out_specs=(anywhere, anywhere),
            scratch_shapes=[
                pltpu.VMEM((rows, rank), bf16),
                pltpu.VMEM((steps, cols, rank), bf16),
                pltpu.VMEM((steps, cols, rank), bf16),
                pltpu.VMEM((steps, cols, rows), bf16),
                pltpu.VMEM((rows, rank), f32),
                pltpu.VMEM((rows // 2, rank), bf16),
                pltpu.VMEM((rows // 2, rank), bf16),
                pltpu.VMEM((rows // 2, rank), bf16),
                pltpu.VMEM((others, rows // 2, rank), bf16),
                pltpu.VMEM((rows, rank), bf16),
                dma((2 + steps,)),
                dma((steps - 1, CHUNKS)),
                dma((steps - 1, CHUNKS)),
                dma((CHUNKS,)),
                dma((PIECES,)),
                dma((PIECES,)),
                dma((others, PIECES)),
                dma((others, PIECES)),
                dma((PIECES,)),
                dma((PIECES,)),
                dma((2,)),
            ],
            compiler_params=pltpu.CompilerParams(
                collective_id=0, has_side_effects=True, vmem_limit_bytes=48 * 1024 * 1024
            ),
        )(
            left_factor, right_factor, observed,
            row_codes.reshape(1, rows), shift_codes.reshape(steps, CHUNKS, size),
        )

    in_specs = (
        P("blk", None),
        P("lane", "blk", None),
        P("lane", None, None, "blk"),
        P("blk"),
        P("lane", None, "blk"),
    )
    out_specs = (P("blk", None), P("lane", "blk", None))
    return jax.shard_map(local, mesh=mesh, in_specs=in_specs, out_specs=out_specs, check_vma=False)
```

```python
import functools
import math

import jax
import jax.numpy as jnp
from jax import lax
from jax.experimental import pallas as pl
from jax.experimental.pallas import tpu as pltpu
from jax.sharding import PartitionSpec as P

step_right = 0.25
step_left = 0.1

CHUNKS = 4
PIECES = 4
MESH = pl.DeviceIdType.MESH


def kernel(
    blocks, lanes,
    left_hbm, right_hbm, obs_hbm, codes_ref, shift_ref,
    left_out, right_out,
    left, visited, updated, obs, grad, pair_out, pair_in, peer_out, peer_in, result,
    load_sem, send_sem, recv_sem, store_sem, pair_send, pair_recv, peer_send, peer_recv, last_send, last_recv, out_sem,
):
    steps, cols, rows = obs.shape
    rank = left.shape[1]
    scale = 1.0 / math.sqrt(rank)
    size = cols // CHUNKS
    half = rows // 2
    part = half // PIECES
    blk = lax.axis_index("blk")
    lane = lax.axis_index("lane")
    ahead = lax.rem(blk + 1, blocks)
    behind = lax.rem(blk + blocks - 1, blocks)
    side = lax.rem(lane, 2)
    pair = lane + 1 - 2 * side
    peers = [lax.rem(lane + 2 * hop, lanes) for hop in range(1, lanes // 2)]

    loads = [
        pltpu.make_async_copy(left_hbm, left, load_sem.at[0]),
        pltpu.make_async_copy(right_hbm.at[0], visited.at[0], load_sem.at[1]),
    ]
    for s in range(steps):
        loads.append(pltpu.make_async_copy(obs_hbm.at[0, s], obs.at[s], load_sem.at[2 + s]))
    for copy in loads:
        copy.start()

    barrier = pltpu.get_barrier_semaphore()
    for neighbour in (behind, ahead):
        pl.semaphore_signal(barrier, inc=1, device_id={"blk": neighbour}, device_id_type=MESH)
    for friend in [pair] + peers:
        pl.semaphore_signal(barrier, inc=1, device_id={"lane": friend}, device_id_type=MESH)
    pl.semaphore_wait(barrier, 2 + 1 + len(peers))

    grad[...] = jnp.zeros_like(grad)
    loads[0].wait()
    loads[1].wait()

    def hop(s, k):
        span = pl.ds(pl.multiple_of(k * size, size), size)
        return pltpu.make_async_remote_copy(
            src_ref=updated.at[s, span],
            dst_ref=visited.at[s + 1, span],
            send_sem=send_sem.at[s, k],
            recv_sem=recv_sem.at[s, k],
            device_id={"blk": ahead},
            device_id_type=MESH,
        )

    def keep(k):
        span = pl.ds(pl.multiple_of(k * size, size), size)
        return pltpu.make_async_copy(updated.at[steps - 1, span], right_out.at[0, span], store_sem.at[k])

    for s in range(steps):
        loads[2 + s].wait()

        @pl.loop(0, CHUNKS)
        def _(k):
            span = pl.ds(pl.multiple_of(k * size, size), size)
            shifts = jnp.transpose(jnp.broadcast_to(shift_ref[0, pl.ds(s, 1), span], (size, size)))
            shifts = jnp.concatenate([shifts] * (rows // size), axis=1)
            seen = (jnp.right_shift(codes_ref[...], shifts) & 1) == 1
            if s > 0:
                hop(s - 1, k).wait_recv()
            block = visited[s, span, :]
            predicted = lax.dot_general(
                block, left[...], (((1,), (1,)), ((), ())), preferred_element_type=jnp.float32
            )
            error = predicted * scale - obs[s, span, :].astype(jnp.float32)
            error = jnp.where(seen, error, 0.0).astype(jnp.bfloat16)
            move = jnp.dot(error, left[...], preferred_element_type=jnp.float32)
            updated[s, span, :] = (block.astype(jnp.float32) - step_right * scale * move).astype(jnp.bfloat16)
            if s + 1 < steps:
                hop(s, k).start()
            else:
                keep(k).start()
            grad[...] += lax.dot_general(
                error, block, (((0,), (0,)), ((), ())), preferred_element_type=jnp.float32
            )

    mine = pl.multiple_of(side * half, half)
    other = pl.multiple_of((1 - side) * half, half)

    def swap(q):
        span = pl.ds(q * part, part)
        return pltpu.make_async_remote_copy(
            src_ref=pair_out.at[span], dst_ref=pair_in.at[span],
            send_sem=pair_send.at[q], recv_sem=pair_recv.at[q],
            device_id={"lane": pair}, device_id_type=MESH,
        )

    def cross(m, q):
        span = pl.ds(q * part, part)
        return pltpu.make_async_remote_copy(
            src_ref=peer_out.at[span], dst_ref=peer_in.at[m, span],
            send_sem=peer_send.at[m, q], recv_sem=peer_recv.at[m, q],
            device_id={"lane": peers[m]}, device_id_type=MESH,
        )

    def share(q):
        span = pl.ds(pl.multiple_of(mine + q * part, part), part)
        return pltpu.make_async_remote_copy(
            src_ref=result.at[span], dst_ref=result.at[span],
            send_sem=last_send.at[q], recv_sem=last_recv.at[q],
            device_id={"lane": pair}, device_id_type=MESH,
        )

    for q in range(PIECES):
        pair_out[pl.ds(q * part, part), :] = grad[pl.ds(pl.multiple_of(other + q * part, part), part), :].astype(jnp.bfloat16)
        swap(q).start()
    for q in range(PIECES):
        span = pl.ds(q * part, part)
        swap(q).wait_recv()
        peer_out[span, :] = (
            grad[pl.ds(pl.multiple_of(mine + q * part, part), part), :] + pair_in[span, :].astype(jnp.float32)
        ).astype(jnp.bfloat16)
        for m in range(len(peers)):
            cross(m, q).start()
    for q in range(PIECES):
        span = pl.ds(q * part, part)
        here = pl.ds(pl.multiple_of(mine + q * part, part), part)
        total = peer_out[span, :].astype(jnp.float32)
        for m in range(len(peers)):
            cross(m, q).wait_recv()
            total = total + peer_in[m, span, :].astype(jnp.float32)
        result[here, :] = (left[here, :].astype(jnp.float32) - step_left * scale * total).astype(jnp.bfloat16)
        share(q).start()
    own = pltpu.make_async_copy(result.at[pl.ds(mine, half)], left_out.at[pl.ds(mine, half)], out_sem.at[0])
    own.start()
    for q in range(PIECES):
        share(q).wait_recv()
    theirs = pltpu.make_async_copy(result.at[pl.ds(other, half)], left_out.at[pl.ds(other, half)], out_sem.at[1])
    theirs.start()
    for s in range(steps - 1):
        @pl.loop(0, CHUNKS)
        def _(k):
            hop(s, k).wait_send()

    @pl.loop(0, CHUNKS)
    def _(k):
        keep(k).wait()

    for q in range(PIECES):
        swap(q).wait_send()
        for m in range(len(peers)):
            cross(m, q).wait_send()
        share(q).wait_send()
    own.wait()
    theirs.wait()


def solution(mesh):
    blocks = mesh.shape["blk"]
    lanes = mesh.shape["lane"]

    def local(left_factor, right_factor, observed, row_codes, shift_codes):
        rows, rank = left_factor.shape
        _, steps, cols, _ = observed.shape
        size = cols // CHUNKS
        bf16, f32 = jnp.bfloat16, jnp.float32
        dma = pltpu.SemaphoreType.DMA
        anywhere = pl.BlockSpec(memory_space=pl.ANY)
        vmem = pl.BlockSpec(memory_space=pltpu.VMEM)
        others = lanes // 2 - 1
        return pl.pallas_call(
            functools.partial(kernel, blocks, lanes),
            out_shape=(
                jax.ShapeDtypeStruct((rows, rank), bf16),
                jax.ShapeDtypeStruct((1, cols, rank), bf16),
            ),
            in_specs=[anywhere, anywhere, anywhere, vmem, vmem],
            out_specs=(anywhere, anywhere),
            scratch_shapes=[
                pltpu.VMEM((rows, rank), bf16),
                pltpu.VMEM((steps, cols, rank), bf16),
                pltpu.VMEM((steps, cols, rank), bf16),
                pltpu.VMEM((steps, cols, rows), bf16),
                pltpu.VMEM((rows, rank), f32),
                pltpu.VMEM((rows // 2, rank), bf16),
                pltpu.VMEM((rows // 2, rank), bf16),
                pltpu.VMEM((rows // 2, rank), bf16),
                pltpu.VMEM((others, rows // 2, rank), bf16),
                pltpu.VMEM((rows, rank), bf16),
                dma((2 + steps,)),
                dma((steps - 1, CHUNKS)),
                dma((steps - 1, CHUNKS)),
                dma((CHUNKS,)),
                dma((PIECES,)),
                dma((PIECES,)),
                dma((others, PIECES)),
                dma((others, PIECES)),
                dma((PIECES,)),
                dma((PIECES,)),
                dma((2,)),
            ],
            compiler_params=pltpu.CompilerParams(
                collective_id=0, has_side_effects=True, vmem_limit_bytes=67043328
            ),
        )(
            left_factor, right_factor, observed,
            row_codes.reshape(1, rows), shift_codes,
        )

    in_specs = (
        P("blk", None),
        P("lane", "blk", None),
        P("lane", None, None, "blk"),
        P("blk"),
        P("lane", None, "blk"),
    )
    out_specs = (P("blk", None), P("lane", "blk", None))
    return jax.shard_map(local, mesh=mesh, in_specs=in_specs, out_specs=out_specs, check_vma=False)
```

```python
import functools
import math

import jax
import jax.numpy as jnp
from jax import lax
from jax.experimental import pallas as pl
from jax.experimental.pallas import tpu as pltpu
from jax.sharding import PartitionSpec as P

step_right = 0.25
step_left = 0.1

CHUNKS = 4
WIDTH = 128
PARTS = 2
PIECES = 4
MESH = pl.DeviceIdType.MESH


def kernel(
    blocks, lanes,
    left_hbm, right_hbm, obs_hbm, codes_hbm, shift_hbm,
    left_out, right_out,
    left, visited, updated, obs, codes, shift, turned, errors, grad, pair_out, pair_in, peer_out, peer_in, result,
    load_sem, send_sem, recv_sem, pair_send, pair_recv, peer_send, peer_recv, last_send, last_recv, out_sem,
):
    steps, cols, rows = obs.shape
    rank = left.shape[1]
    scale = 1.0 / math.sqrt(rank)
    size = cols // CHUNKS
    half = rows // 2
    part = half // PIECES
    width = turned.shape[1]
    blk = lax.axis_index("blk")
    lane = lax.axis_index("lane")
    ahead = lax.rem(blk + 1, blocks)
    behind = lax.rem(blk + blocks - 1, blocks)
    side = lax.rem(lane, 2)
    pair = lane + 1 - 2 * side
    peers = [lax.rem(lane + 2 * hop, lanes) for hop in range(1, lanes // 2)]
    mine = pl.multiple_of(side * half, half)
    other = pl.multiple_of((1 - side) * half, half)

    barrier = pltpu.get_barrier_semaphore()
    for neighbour in (behind, ahead):
        pl.semaphore_signal(barrier, inc=1, device_id={"blk": neighbour}, device_id_type=MESH)
    for friend in [pair] + peers:
        pl.semaphore_signal(barrier, inc=1, device_id={"lane": friend}, device_id_type=MESH)

    loads = [
        pltpu.make_async_copy(shift_hbm, shift, load_sem.at[0]),
        pltpu.make_async_copy(codes_hbm, codes, load_sem.at[1]),
        pltpu.make_async_copy(right_hbm.at[0], visited.at[0], load_sem.at[2]),
        pltpu.make_async_copy(left_hbm, left, load_sem.at[3]),
    ]
    for s in range(steps):
        loads.append(pltpu.make_async_copy(obs_hbm.at[0, s], obs.at[s], load_sem.at[4 + s]))
    for copy in loads:
        copy.start()

    def hop(s, k):
        span = pl.ds(pl.multiple_of(k * size, size), size)
        return pltpu.make_async_remote_copy(
            src_ref=updated.at[s, span],
            dst_ref=visited.at[s + 1, span],
            send_sem=send_sem.at[s, k],
            recv_sem=recv_sem.at[s, k],
            device_id={"blk": ahead},
            device_id_type=MESH,
        )

    def turn(s):
        for first in range(0, cols, width):
            span = pl.ds(first, width)
            turned[span, :] = jnp.transpose(jnp.broadcast_to(shift[0, pl.ds(s, 1), span], (width, width)))

    def error_of(s, k):
        span = pl.ds(pl.multiple_of(k * size, size), size)
        shifts = jnp.concatenate([turned[span, :]] * (rows // width), axis=1)
        seen = (jnp.right_shift(codes[...], shifts) & 1) == 1
        predicted = lax.dot_general(
            visited[s, span, :], left[...], (((1,), (1,)), ((), ())), preferred_element_type=jnp.float32
        )
        error = predicted * scale - obs[s, span, :].astype(jnp.float32)
        return jnp.where(seen, error, 0.0).astype(jnp.bfloat16)

    def stepped(error, block):
        move = jnp.dot(error, left[...], preferred_element_type=jnp.float32)
        return (block.astype(jnp.float32) - step_right * scale * move).astype(jnp.bfloat16)

    def add_left(error, block):
        grad[...] += lax.dot_general(
            error, block, (((0,), (0,)), ((), ())), preferred_element_type=jnp.float32
        )

    def visit(s, k, before_send=None):
        span = pl.ds(pl.multiple_of(k * size, size), size)
        if s > 0:
            hop(s - 1, k).wait_recv()
        error = error_of(s, k)
        block = visited[s, span, :]
        updated[s, span, :] = stepped(error, block)
        if before_send is not None:
            before_send()
        hop(s, k).start()
        add_left(error, block)

    loads[0].wait()
    turn(0)
    grad[...] = jnp.zeros_like(grad)
    for copy in loads[1:5]:
        copy.wait()
    visit(0, 0, lambda: pl.semaphore_wait(barrier, 2 + 1 + len(peers)))
    for s in range(steps - 1):
        if s > 0:
            loads[4 + s].wait()
            turn(s)
        pl.loop(1 if s == 0 else 0, CHUNKS)(functools.partial(visit, s))

    last = steps - 1
    loads[4 + last].wait()
    turn(last)

    @pl.loop(0, CHUNKS - 1)
    def _(k):
        span = pl.ds(pl.multiple_of(k * size, size), size)
        hop(last - 1, k).wait_recv()
        error = error_of(last, k)
        errors[span, :] = error
        add_left(error, visited[last, span, :])

    tail = pl.ds((CHUNKS - 1) * size, size)
    hop(last - 1, CHUNKS - 1).wait_recv()
    errors[tail, :] = error_of(last, CHUNKS - 1)

    def finish(first):
        span = pl.ds(first, half)
        return grad[span, :] + lax.dot_general(
            errors[tail, span], visited[last, tail, :], (((0,), (0,)), ((), ())), preferred_element_type=jnp.float32
        )

    def swap(q):
        span = pl.ds(q * part, part)
        return pltpu.make_async_remote_copy(
            src_ref=pair_out.at[span], dst_ref=pair_in.at[span],
            send_sem=pair_send.at[q], recv_sem=pair_recv.at[q],
            device_id={"lane": pair}, device_id_type=MESH,
        )

    def cross(m, q):
        span = pl.ds(q * part, part)
        return pltpu.make_async_remote_copy(
            src_ref=peer_out.at[span], dst_ref=peer_in.at[m, span],
            send_sem=peer_send.at[m, q], recv_sem=peer_recv.at[m, q],
            device_id={"lane": peers[m]}, device_id_type=MESH,
        )

    def share(q):
        span = pl.ds(pl.multiple_of(mine + q * part, part), part)
        return pltpu.make_async_remote_copy(
            src_ref=result.at[span], dst_ref=result.at[span],
            send_sem=last_send.at[q], recv_sem=last_recv.at[q],
            device_id={"lane": pair}, device_id_type=MESH,
        )

    pair_out[...] = finish(other).astype(jnp.bfloat16)
    for q in range(PIECES):
        swap(q).start()
    grad[pl.ds(mine, half), :] = finish(mine)
    for q in range(PIECES):
        span = pl.ds(q * part, part)
        swap(q).wait_recv()
        peer_out[span, :] = (
            grad[pl.ds(pl.multiple_of(mine + q * part, part), part), :] + pair_in[span, :].astype(jnp.float32)
        ).astype(jnp.bfloat16)
        for m in range(len(peers)):
            cross(m, q).start()

    @pl.loop(0, CHUNKS)
    def _(k):
        span = pl.ds(pl.multiple_of(k * size, size), size)
        updated[last, span, :] = stepped(errors[span, :], visited[last, span, :])

    outs = [
        pltpu.make_async_copy(updated.at[last], right_out.at[0], out_sem.at[0]),
        pltpu.make_async_copy(result.at[pl.ds(mine, half)], left_out.at[pl.ds(mine, half)], out_sem.at[1]),
        pltpu.make_async_copy(result.at[pl.ds(other, half)], left_out.at[pl.ds(other, half)], out_sem.at[2]),
    ]
    outs[0].start()
    for s in range(steps - 1):
        @pl.loop(0, CHUNKS)
        def _(k):
            hop(s, k).wait_send()

    for q in range(PIECES):
        span = pl.ds(q * part, part)
        here = pl.ds(pl.multiple_of(mine + q * part, part), part)
        total = peer_out[span, :].astype(jnp.float32)
        for m in range(len(peers)):
            cross(m, q).wait_recv()
            total = total + peer_in[m, span, :].astype(jnp.float32)
        result[here, :] = (left[here, :].astype(jnp.float32) - step_left * scale * total).astype(jnp.bfloat16)
        share(q).start()
    outs[1].start()
    for q in range(PIECES):
        share(q).wait_recv()
    outs[2].start()
    for q in range(PIECES):
        swap(q).wait_send()
        for m in range(len(peers)):
            cross(m, q).wait_send()
        share(q).wait_send()
    for copy in outs:
        copy.wait()


def place(left_from, right_from, left_to, right_to, held, in_sem, out_sem):
    pairs = [(left_from, left_to), (right_from.at[0], right_to.at[0])]
    rows = left_from.shape[0] // PARTS
    moves = []
    for which, (source, target) in enumerate(pairs):
        for p in range(PARTS):
            span = pl.ds(p * rows, rows)
            moves.append((
                pltpu.make_async_copy(source.at[span], held.at[which, span], in_sem.at[which, p]),
                pltpu.make_async_copy(held.at[which, span], target.at[span], out_sem.at[which, p]),
            ))
    for inward, _ in moves:
        inward.start()
    for inward, outward in moves:
        inward.wait()
        outward.start()
    for _, outward in moves:
        outward.wait()


def solution(mesh):
    blocks = mesh.shape["blk"]
    lanes = mesh.shape["lane"]

    def local(left_factor, right_factor, observed, row_codes, shift_codes):
        rows, rank = left_factor.shape
        _, steps, cols, _ = observed.shape
        bf16, f32 = jnp.bfloat16, jnp.float32
        dma = pltpu.SemaphoreType.DMA
        hbm = pl.BlockSpec(memory_space=pltpu.HBM)
        others = lanes // 2 - 1
        shapes = (
            jax.ShapeDtypeStruct((rows, rank), bf16),
            jax.ShapeDtypeStruct((1, cols, rank), bf16),
        )
        results = pl.pallas_call(
            functools.partial(kernel, blocks, lanes),
            out_shape=shapes,
            in_specs=[hbm] * 5,
            out_specs=(hbm, hbm),
            scratch_shapes=[
                pltpu.VMEM((rows, rank), bf16),
                pltpu.VMEM((steps, cols, rank), bf16),
                pltpu.VMEM((steps, cols, rank), bf16),
                pltpu.VMEM((steps, cols, rows), bf16),
                pltpu.VMEM((1, rows), jnp.int32),
                pltpu.VMEM((1, steps, cols), jnp.int32),
                pltpu.VMEM((cols, WIDTH), jnp.int32),
                pltpu.VMEM((cols, rows), bf16),
                pltpu.VMEM((rows, rank), f32),
                pltpu.VMEM((rows // 2, rank), bf16),
                pltpu.VMEM((rows // 2, rank), bf16),
                pltpu.VMEM((rows // 2, rank), bf16),
                pltpu.VMEM((others, rows // 2, rank), bf16),
                pltpu.VMEM((rows, rank), bf16),
                dma((4 + steps,)),
                dma((steps - 1, CHUNKS)),
                dma((steps - 1, CHUNKS)),
                dma((PIECES,)),
                dma((PIECES,)),
                dma((others, PIECES)),
                dma((others, PIECES)),
                dma((PIECES,)),
                dma((PIECES,)),
                dma((3,)),
            ],
            compiler_params=pltpu.CompilerParams(
                collective_id=0, has_side_effects=True, vmem_limit_bytes=67043328
            ),
        )(
            left_factor, right_factor, observed,
            row_codes.reshape(1, rows), shift_codes,
        )
        return pl.pallas_call(
            place,
            out_shape=shapes,
            in_specs=[hbm] * 2,
            out_specs=(hbm, hbm),
            scratch_shapes=[pltpu.VMEM((2, max(rows, cols), rank), bf16), dma((2, PARTS)), dma((2, PARTS))],
            compiler_params=pltpu.CompilerParams(vmem_limit_bytes=67043328),
        )(*results)

    in_specs = (
        P("blk", None),
        P("lane", "blk", None),
        P("lane", None, None, "blk"),
        P("blk"),
        P("lane", None, "blk"),
    )
    out_specs = (P("blk", None), P("lane", "blk", None))
    return jax.shard_map(local, mesh=mesh, in_specs=in_specs, out_specs=out_specs, check_vma=False)
```

```python
import functools
import math

import jax
import jax.numpy as jnp
from jax import lax
from jax.experimental import pallas as pl
from jax.experimental.pallas import tpu as pltpu
from jax.sharding import PartitionSpec as P

step_right = 0.25
step_left = 0.1

CHUNKS = 4
WIDTH = 128
PARTS = 2
PIECES = 4
MESH = pl.DeviceIdType.MESH


def kernel(
    blocks, lanes,
    left_hbm, right_hbm, obs_hbm, codes_hbm, shift_hbm,
    left_out, right_out,
    left, visited, updated, obs, codes, shift, turned, errors, grad, pair_out, pair_in, peer_out, peer_in, result,
    load_sem, send_sem, recv_sem, pair_send, pair_recv, peer_send, peer_recv, last_send, last_recv, out_sem,
):
    steps, cols, rows = obs.shape
    rank = left.shape[1]
    scale = 1.0 / math.sqrt(rank)
    size = cols // CHUNKS
    half = rows // 2
    part = half // PIECES
    width = turned.shape[1]
    blk = lax.axis_index("blk")
    lane = lax.axis_index("lane")
    ahead = lax.rem(blk + 1, blocks)
    behind = lax.rem(blk + blocks - 1, blocks)
    side = lax.rem(lane, 2)
    pair = lane + 1 - 2 * side
    peers = [lax.rem(lane + 2 * hop, lanes) for hop in range(1, lanes // 2)]
    mine = pl.multiple_of(side * half, half)
    other = pl.multiple_of((1 - side) * half, half)

    barrier = pltpu.get_barrier_semaphore()
    pl.semaphore_signal(barrier, inc=1, device_id={"blk": behind}, device_id_type=MESH)
    for friend in [pair] + peers:
        pl.semaphore_signal(barrier, inc=1, device_id={"lane": friend}, device_id_type=MESH)

    loads = [
        pltpu.make_async_copy(shift_hbm, shift, load_sem.at[0]),
        pltpu.make_async_copy(codes_hbm, codes, load_sem.at[1]),
        pltpu.make_async_copy(right_hbm.at[0], visited.at[0], load_sem.at[2]),
        pltpu.make_async_copy(left_hbm, left, load_sem.at[3]),
    ]
    for s in range(steps):
        loads.append(pltpu.make_async_copy(obs_hbm.at[0, s], obs.at[s], load_sem.at[4 + s]))
    for copy in loads[:5]:
        copy.start()

    def hop(s, k):
        span = pl.ds(pl.multiple_of(k * size, size), size)
        return pltpu.make_async_remote_copy(
            src_ref=updated.at[s, span],
            dst_ref=visited.at[s + 1, span],
            send_sem=send_sem.at[s, k],
            recv_sem=recv_sem.at[s, k],
            device_id={"blk": ahead},
            device_id_type=MESH,
        )

    def turn(s):
        for first in range(0, cols, width):
            span = pl.ds(first, width)
            turned[span, :] = jnp.transpose(jnp.broadcast_to(shift[0, pl.ds(s, 1), span], (width, width)))

    def error_of(s, k):
        span = pl.ds(pl.multiple_of(k * size, size), size)
        shifts = jnp.concatenate([turned[span, :]] * (rows // width), axis=1)
        seen = (jnp.right_shift(codes[...], shifts) & 1) == 1
        predicted = lax.dot_general(
            visited[s, span, :], left[...], (((1,), (1,)), ((), ())), preferred_element_type=jnp.float32
        )
        error = predicted * scale - obs[s, span, :].astype(jnp.float32)
        return jnp.where(seen, error, 0.0).astype(jnp.bfloat16)

    def stepped(error, block):
        move = jnp.dot(error, left[...], preferred_element_type=jnp.float32)
        return (block.astype(jnp.float32) - step_right * scale * move).astype(jnp.bfloat16)

    def add_left(error, block):
        grad[...] += lax.dot_general(
            error, block, (((0,), (0,)), ((), ())), preferred_element_type=jnp.float32
        )

    def visit(s, k, before_send=None):
        span = pl.ds(pl.multiple_of(k * size, size), size)
        if s > 0:
            hop(s - 1, k).wait_recv()
        error = error_of(s, k)
        block = visited[s, span, :]
        updated[s, span, :] = stepped(error, block)
        if before_send is not None:
            before_send()
        hop(s, k).start()
        add_left(error, block)

    grad[...] = jnp.zeros_like(grad)
    loads[0].wait()
    turn(0)
    for copy in loads[1:5]:
        copy.wait()
    visit(0, 0, lambda: pl.semaphore_wait(barrier, 2 + len(peers)))
    for copy in loads[5:]:
        copy.start()
    for s in range(steps - 1):
        if s > 0:
            loads[4 + s].wait()
            turn(s)
        pl.loop(1 if s == 0 else 0, CHUNKS)(functools.partial(visit, s))

    last = steps - 1
    loads[4 + last].wait()
    turn(last)

    @pl.loop(0, CHUNKS - 1)
    def _(k):
        span = pl.ds(pl.multiple_of(k * size, size), size)
        hop(last - 1, k).wait_recv()
        error = error_of(last, k)
        errors[span, :] = error
        add_left(error, visited[last, span, :])

    tail = pl.ds((CHUNKS - 1) * size, size)
    hop(last - 1, CHUNKS - 1).wait_recv()
    errors[tail, :] = error_of(last, CHUNKS - 1)

    def finish(first):
        span = pl.ds(first, half)
        return grad[span, :] + lax.dot_general(
            errors[tail, span], visited[last, tail, :], (((0,), (0,)), ((), ())), preferred_element_type=jnp.float32
        )

    def swap(q):
        span = pl.ds(q * part, part)
        return pltpu.make_async_remote_copy(
            src_ref=pair_out.at[span], dst_ref=pair_in.at[span],
            send_sem=pair_send.at[q], recv_sem=pair_recv.at[q],
            device_id={"lane": pair}, device_id_type=MESH,
        )

    def cross(m, q):
        span = pl.ds(q * part, part)
        return pltpu.make_async_remote_copy(
            src_ref=peer_out.at[span], dst_ref=peer_in.at[m, span],
            send_sem=peer_send.at[m, q], recv_sem=peer_recv.at[m, q],
            device_id={"lane": peers[m]}, device_id_type=MESH,
        )

    def share(q):
        span = pl.ds(pl.multiple_of(mine + q * part, part), part)
        return pltpu.make_async_remote_copy(
            src_ref=result.at[span], dst_ref=result.at[span],
            send_sem=last_send.at[q], recv_sem=last_recv.at[q],
            device_id={"lane": pair}, device_id_type=MESH,
        )

    pair_out[...] = finish(other).astype(jnp.bfloat16)
    for q in range(PIECES):
        swap(q).start()
    grad[pl.ds(mine, half), :] = finish(mine)
    for q in range(PIECES):
        span = pl.ds(q * part, part)
        swap(q).wait_recv()
        peer_out[span, :] = (
            grad[pl.ds(pl.multiple_of(mine + q * part, part), part), :] + pair_in[span, :].astype(jnp.float32)
        ).astype(jnp.bfloat16)
        for m in range(len(peers)):
            cross(m, q).start()

    @pl.loop(0, CHUNKS)
    def _(k):
        span = pl.ds(pl.multiple_of(k * size, size), size)
        updated[last, span, :] = stepped(errors[span, :], visited[last, span, :])

    outs = [
        pltpu.make_async_copy(updated.at[last], right_out.at[0], out_sem.at[0]),
        pltpu.make_async_copy(result.at[pl.ds(mine, half)], left_out.at[pl.ds(mine, half)], out_sem.at[1]),
        pltpu.make_async_copy(result.at[pl.ds(other, half)], left_out.at[pl.ds(other, half)], out_sem.at[2]),
    ]
    outs[0].start()
    for s in range(steps - 1):
        @pl.loop(0, CHUNKS)
        def _(k):
            hop(s, k).wait_send()

    for q in range(PIECES):
        span = pl.ds(q * part, part)
        here = pl.ds(pl.multiple_of(mine + q * part, part), part)
        total = peer_out[span, :].astype(jnp.float32)
        for m in range(len(peers)):
            cross(m, q).wait_recv()
            total = total + peer_in[m, span, :].astype(jnp.float32)
        result[here, :] = (left[here, :].astype(jnp.float32) - step_left * scale * total).astype(jnp.bfloat16)
        share(q).start()
    outs[1].start()
    for q in range(PIECES):
        share(q).wait_recv()
    outs[2].start()
    for q in range(PIECES):
        swap(q).wait_send()
        for m in range(len(peers)):
            cross(m, q).wait_send()
        share(q).wait_send()
    for copy in outs:
        copy.wait()


def place(left_from, right_from, left_to, right_to, held, in_sem, out_sem):
    pairs = [(left_from, left_to), (right_from.at[0], right_to.at[0])]
    rows = left_from.shape[0] // PARTS
    moves = []
    for which, (source, target) in enumerate(pairs):
        for p in range(PARTS):
            span = pl.ds(p * rows, rows)
            moves.append((
                pltpu.make_async_copy(source.at[span], held.at[which, span], in_sem.at[which, p]),
                pltpu.make_async_copy(held.at[which, span], target.at[span], out_sem.at[which, p]),
            ))
    for inward, _ in moves:
        inward.start()
    for inward, outward in moves:
        inward.wait()
        outward.start()
    for _, outward in moves:
        outward.wait()


def solution(mesh):
    blocks = mesh.shape["blk"]
    lanes = mesh.shape["lane"]

    def local(left_factor, right_factor, observed, row_codes, shift_codes):
        rows, rank = left_factor.shape
        _, steps, cols, _ = observed.shape
        bf16, f32 = jnp.bfloat16, jnp.float32
        dma = pltpu.SemaphoreType.DMA
        hbm = pl.BlockSpec(memory_space=pltpu.HBM)
        others = lanes // 2 - 1
        shapes = (
            jax.ShapeDtypeStruct((rows, rank), bf16),
            jax.ShapeDtypeStruct((1, cols, rank), bf16),
        )
        results = pl.pallas_call(
            functools.partial(kernel, blocks, lanes),
            out_shape=shapes,
            in_specs=[hbm] * 5,
            out_specs=(hbm, hbm),
            scratch_shapes=[
                pltpu.VMEM((rows, rank), bf16),
                pltpu.VMEM((steps, cols, rank), bf16),
                pltpu.VMEM((steps, cols, rank), bf16),
                pltpu.VMEM((steps, cols, rows), bf16),
                pltpu.VMEM((1, rows), jnp.int32),
                pltpu.VMEM((1, steps, cols), jnp.int32),
                pltpu.VMEM((cols, WIDTH), jnp.int32),
                pltpu.VMEM((cols, rows), bf16),
                pltpu.VMEM((rows, rank), f32),
                pltpu.VMEM((rows // 2, rank), bf16),
                pltpu.VMEM((rows // 2, rank), bf16),
                pltpu.VMEM((rows // 2, rank), bf16),
                pltpu.VMEM((others, rows // 2, rank), bf16),
                pltpu.VMEM((rows, rank), bf16),
                dma((4 + steps,)),
                dma((steps - 1, CHUNKS)),
                dma((steps - 1, CHUNKS)),
                dma((PIECES,)),
                dma((PIECES,)),
                dma((others, PIECES)),
                dma((others, PIECES)),
                dma((PIECES,)),
                dma((PIECES,)),
                dma((3,)),
            ],
            compiler_params=pltpu.CompilerParams(
                collective_id=0, has_side_effects=True, vmem_limit_bytes=67043328
            ),
        )(
            left_factor, right_factor, observed,
            row_codes.reshape(1, rows), shift_codes,
        )
        return pl.pallas_call(
            place,
            out_shape=shapes,
            in_specs=[hbm] * 2,
            out_specs=(hbm, hbm),
            scratch_shapes=[pltpu.VMEM((2, max(rows, cols), rank), bf16), dma((2, PARTS)), dma((2, PARTS))],
            compiler_params=pltpu.CompilerParams(vmem_limit_bytes=67043328),
        )(*results)

    in_specs = (
        P("blk", None),
        P("lane", "blk", None),
        P("lane", None, None, "blk"),
        P("blk"),
        P("lane", None, "blk"),
    )
    out_specs = (P("blk", None), P("lane", "blk", None))
    return jax.shard_map(local, mesh=mesh, in_specs=in_specs, out_specs=out_specs, check_vma=False)
```
